32 devices in a mesh: epoch: 8 (over z, y), blend: 4 (over x, core).
Axes of the slice: x: 2, y: 2, z: 4, core: 2. Of those that a mesh axis runs over, the one named last changes fastest.
Arguments:
- models: float32 [4, 16, 6, 4096], P('blend', 'epoch'), may hold values from -6 to 6
- observed: bfloat16 [8, 64, 4096], P('epoch', 'blend'), may hold values from -6 to 6
- weights: float32 [8, 64], P('epoch', 'blend'), may hold values from 0.5 to 2
- coverage: int32 [8, 64], P('epoch', 'blend'), may hold values from 0 to 1, as said below
- offsets: int32 [8, 64, 2], P('epoch', 'blend'), may hold values from 0 to 63
- counts: int32 [4, 16], P('blend', 'epoch'), may hold values from 1 to 8, as said below
- psf_y: bfloat16 [8, 4096], P('epoch'), may hold values from -0.75 to 0.75
- resample_y: bfloat16 [8, 4096], P('epoch'), may hold values from -0.75 to 0.75
- psf_x: bfloat16 [8, 4096], P('epoch'), may hold values from -0.75 to 0.75
- resample_x: bfloat16 [8, 4096], P('epoch'), may hold values from -0.75 to 0.75
Outputs:
- updated: float32 [4, 16, 6, 4096], P('blend', 'epoch')
The draws below stay inside these ranges and needn't reach their ends.
Inputs may be any that keep to these rules, and one draw needn't show every extreme that they name: `coverage`: every blend is seen by one epoch or more. counts of blend b is the sum of coverage over all epochs for b.
All inputs are finite; a program needn't handle non-finite values.
Results may differ from the reference program's by a relative error of at most 0.0017.
Values may be sent and summed in bfloat16 or wider, within the bound.
A program may use at most 128 MiB of HBM per device.

```python
import math
import jax
import jax.numpy as jnp
from jax import lax

CUT = 64
BANDS = 6
PIX2 = 4096
E = 8
BLEND_GRP = 16
B = 64
N_BLEND = 4


def coverage_table(key):
    inner = jax.random.fold_in(key, 11)
    chance = jax.random.randint(jax.random.fold_in(inner, 1), (B,), 10, 95)
    rolled = jax.random.randint(jax.random.fold_in(inner, 2), (E, B), 0, 100)
    seen = rolled < chance[None, :]
    forced = jnp.arange(E, dtype=jnp.int32)[:, None] == jnp.arange(B, dtype=jnp.int32)[None, :] % E
    return jnp.logical_or(seen, forced).astype(jnp.int32)


def draw_coverage(key, part):
    return coverage_table(key)


def draw_counts(key, part):
    return jnp.sum(coverage_table(key), axis=0).astype(jnp.int32).reshape(N_BLEND, BLEND_GRP)


def place_ends(values, rng, smallest, top_value):
    longest = values.shape.index(max(values.shape))
    spots = []
    for shift in (0, 1):
        where = [jax.random.randint(jax.random.fold_in(rng, axis), (), 0, length) for axis, length in enumerate(values.shape)]
        where[longest] = (where[longest] + shift) % values.shape[longest]
        spots.append(tuple(where))
    return values.at[spots[0]].set(smallest).at[spots[1]].set(top_value)


def steps_of(stream_key, extent, pieces, smallest, largest):
    gain = 1.0
    for dim, shards_of in pieces:
        heights = jax.random.uniform(jax.random.fold_in(jax.random.fold_in(stream_key, 6), dim), (shards_of,), jnp.float32, smallest / len(pieces), largest / len(pieces))
        gain = gain * jnp.repeat(jnp.exp(heights), extent[dim] // shards_of).reshape((-1,) + (1,) * (len(extent) - 1 - dim))
    return gain


def centred(own_key, dims, deviation, reach, split=(), held_as=jnp.bfloat16):
    array = jax.random.normal(own_key, dims, jnp.float32) * deviation
    if len(split) > 0:
        array = steps_of(own_key, dims, split, -0.22, 0.18) * array
    return jnp.clip(array, min=-reach, max=reach).astype(held_as)


def setup_inputs(seed: int = 0) -> dict:
    arg_keys = jax.random.split(jax.random.key(seed), 11)
    return {
        "models": centred(arg_keys[0], (N_BLEND, BLEND_GRP, BANDS, PIX2), 1.0, 6.0, ((0, 4), (1, 8)), jnp.float32),
        "observed": centred(arg_keys[1], (E, B, PIX2), 1.0, 6.0, ((0, 8), (1, 4))),
        "weights": jnp.clip(jnp.exp(math.log(2.0) - 1.3862944 * jax.random.uniform(arg_keys[2], (E, B), jnp.float32) ** steps_of(arg_keys[2], (E, B), ((0, 8), (1, 4)), -0.2, 0.2)), 0.5, 2.0),
        "coverage": draw_coverage(jax.random.fold_in(arg_keys[10], 71), 0),
        "offsets": place_ends(jax.random.randint(arg_keys[4], (E, B, 2), 0, CUT), jax.random.fold_in(arg_keys[4], 1), 0, CUT - 1).astype(jnp.int32),
        "counts": draw_counts(jax.random.fold_in(arg_keys[10], 71), 0),
        "psf_y": centred(arg_keys[6], (E, PIX2), CUT ** -0.5, 0.75, ((0, 8),)),
        "resample_y": centred(arg_keys[7], (E, PIX2), CUT ** -0.5, 0.75, ((0, 8),)),
        "psf_x": centred(arg_keys[8], (E, PIX2), CUT ** -0.5, 0.75, ((0, 8),)),
        "resample_x": centred(arg_keys[9], (E, PIX2), CUT ** -0.5, 0.75, ((0, 8),)),
    }


step_size = 0.5


def roll_forward(image, down, across):
    side = image.shape[0]
    doubled = jnp.concatenate([image, image], axis=0)
    rows = lax.dynamic_slice_in_dim(doubled, down, side, 0)
    doubled = jnp.concatenate([rows, rows], axis=1)
    return lax.dynamic_slice_in_dim(doubled, across, side, 1)


def one_epoch(model_low, observed, scale, offsets, left, right, band):
    side = left.shape[0]
    count = observed.shape[0]
    chosen = lax.dynamic_index_in_dim(model_low, band, 1, keepdims=False)
    shifted = jax.vmap(roll_forward)(chosen, offsets[:, 0], offsets[:, 1])
    blurred = jnp.einsum('ij,bjk->bik', left.astype(jnp.float32), shifted.astype(jnp.float32)).astype(jnp.bfloat16)
    predicted = jnp.einsum('bik,lk->bil', blurred.astype(jnp.float32), right.astype(jnp.float32))
    target = observed.reshape(count, side, side).astype(jnp.float32)
    misfit = (scale[:, None, None] * (predicted - target)).astype(jnp.bfloat16)
    back = jnp.einsum('ji,bjk->bik', left.astype(jnp.float32), misfit.astype(jnp.float32)).astype(jnp.bfloat16)
    term = jnp.einsum('bik,kl->bil', back.astype(jnp.float32), right.astype(jnp.float32))
    return jax.vmap(roll_forward)(term, side - offsets[:, 0], side - offsets[:, 1])


def reference(models, observed, weights, coverage, offsets, counts, psf_y, resample_y, psf_x, resample_x):
    flat = models.reshape(B, BANDS, CUT, CUT)
    model_low = flat.astype(jnp.bfloat16)
    lefts = jnp.einsum('eij,ejk->eik', psf_y.reshape(E, CUT, CUT).astype(jnp.float32), resample_y.reshape(E, CUT, CUT).astype(jnp.float32)).astype(jnp.bfloat16)
    rights = jnp.einsum('eij,ejk->eik', psf_x.reshape(E, CUT, CUT).astype(jnp.float32), resample_x.reshape(E, CUT, CUT).astype(jnp.float32)).astype(jnp.bfloat16)
    scale = weights * coverage.astype(jnp.float32)

    def advance(gradient, inputs):
        epoch_id, seen, weight_row, offset_row, left, right = inputs
        band = (epoch_id * BANDS) // E
        term = one_epoch(model_low, seen, weight_row, offset_row, left, right, band)
        current = lax.dynamic_index_in_dim(gradient, band, 0, keepdims=False)
        gradient = lax.dynamic_update_index_in_dim(gradient, current + term, band, 0)
        return gradient, None

    start_grad = jnp.zeros((BANDS, B, CUT, CUT), jnp.float32)
    epochs = jnp.arange(E, dtype=jnp.int32)
    gradient, _ = lax.scan(advance, start_grad, (epochs, observed, scale, offsets, lefts, rights))
    gradient = gradient.transpose(1, 0, 2, 3).reshape(B, BANDS, PIX2)
    divisor = counts.reshape(B).astype(jnp.float32)[:, None, None]
    updated = models.reshape(B, BANDS, PIX2) - step_size * gradient / divisor
    return updated.reshape(N_BLEND, BLEND_GRP, BANDS, PIX2)
```

```python
import functools

import jax
import jax.numpy as jnp
from jax import lax
from jax.experimental import pallas as pl
from jax.experimental.pallas import tpu as pltpu
from jax.sharding import PartitionSpec as P

step_size = 0.5
LANES = 128
UNROLL = 8
MESH = pl.DeviceIdType.MESH


def dot(a, b):
    return jnp.dot(a, b, preferred_element_type=jnp.float32)


def dot_nt(a, b):
    return lax.dot_general(a, b, (((1,), (1,)), ((), ())), preferred_element_type=jnp.float32)


def each(count, body):
    if count <= UNROLL:
        for step in range(count):
            body(step)
    else:

        @pl.loop(0, count)
        def _(step):
            body(step)


def kernel(
    n,
    models_ref,
    obs_ref,
    weight_ref,
    cover_ref,
    off_ref,
    count_ref,
    psf_y_ref,
    res_y_ref,
    psf_x_ref,
    res_x_ref,
    out_ref,
    wide_ref,
    stage_ref,
    tmp_ref,
    target_ref,
    flat_ref,
    square_ref,
    l_ref,
    lt_ref,
    q_ref,
    model_in,
    term_out,
    term_in,
    model_send,
    model_recv,
    term_send,
    term_recv,
):
    bands, side = stage_ref.shape[0], stage_ref.shape[1]
    chunks = psf_y_ref.shape[1] // LANES
    me = lax.axis_index("epoch")

    barrier = pltpu.get_barrier_semaphore()

    def greet(k):
        pl.semaphore_signal(
            barrier, inc=1, device_id={"epoch": lax.rem(me + k + 1, n)}, device_id_type=MESH
        )

    each(n - 1, greet)

    def first_half(rows):
        return lax.broadcasted_iota(jnp.int32, (rows, LANES), 1) < side

    def pair(even, odd):
        low = first_half(even.shape[0])
        return (
            jnp.where(low, even, pltpu.roll(odd, side, 1)),
            jnp.where(low, pltpu.roll(even, side, 1), odd),
        )

    for c in range(bands):
        even = pl.ds(c * side, side // 2, stride=2)
        odd = pl.ds(c * side + 1, side // 2, stride=2)
        wide_ref[even, :], wide_ref[odd, :] = pair(models_ref[even, :], models_ref[odd, :])
        stage_ref[c] = wide_ref[c * side : (c + 1) * side, :].astype(jnp.bfloat16)

    pl.semaphore_wait(barrier, n - 1)

    def model_copy(k):
        dest = lax.rem(me + k, n)
        return pltpu.make_async_remote_copy(
            src_ref=stage_ref.at[dest * bands // n],
            dst_ref=model_in.at[k],
            send_sem=model_send.at[k],
            recv_sem=model_recv.at[k],
            device_id={"epoch": dest},
            device_id_type=MESH,
        )

    def term_copy(k):
        return pltpu.make_async_remote_copy(
            src_ref=term_out.at[k],
            dst_ref=term_in.at[me],
            send_sem=term_send.at[k],
            recv_sem=term_recv.at[me],
            device_id={"epoch": lax.rem(me - k + n, n)},
            device_id_type=MESH,
        )

    each(n - 1, lambda i: model_copy(n - 1 - i).start())

    def square(ref):
        for c in range(chunks):
            flat_ref[c : c + 1, :] = ref[:, c * LANES : (c + 1) * LANES].astype(jnp.float32)
        square_ref[pl.ds(0, chunks, stride=2), :] = flat_ref[:, :side]
        square_ref[pl.ds(1, chunks, stride=2), :] = flat_ref[:, side:]
        return square_ref[...].astype(jnp.bfloat16)

    left = dot(square(psf_y_ref), square(res_y_ref)).astype(jnp.bfloat16)
    right = dot(square(psf_x_ref), square(res_x_ref)).astype(jnp.bfloat16)
    right_twice = jnp.concatenate([right, right], axis=0)
    row = lax.broadcasted_iota(jnp.int32, (2 * side, side), 0)
    col = lax.broadcasted_iota(jnp.int32, (2 * side, side), 1)
    turn = lax.rem(row - col + side, side)
    top = row < side
    diagonal = (lax.broadcasted_iota(jnp.int32, (LANES, LANES), 0) < side) == (
        lax.broadcasted_iota(jnp.int32, (LANES, LANES), 1) < side
    )

    def operators(s):
        def picks(axis):
            moved = jnp.where(top, off_ref[axis, 2 * s], off_ref[axis, 2 * s + 1])
            return jnp.where(turn == moved, 1.0, 0.0).astype(jnp.bfloat16)

        down, across = picks(0), picks(1)
        lt_ref[s] = dot_nt(down, left).astype(jnp.bfloat16)
        l_ref[s, :side] = dot_nt(left, down[:side]).astype(jnp.bfloat16)
        l_ref[s, side:] = dot_nt(left, down[side:]).astype(jnp.bfloat16)
        q_ref[s] = jnp.where(diagonal, dot_nt(across, right_twice), 0.0).astype(jnp.bfloat16)

    each(n, operators)

    for c in range(chunks):
        at = c * 2 * n
        tmp_ref[at : at + 2 * n, :] = obs_ref[:, c * LANES : (c + 1) * LANES].astype(jnp.float32)
        o0 = tmp_ref[pl.ds(at, n, stride=2), :]
        o1 = tmp_ref[pl.ds(at + 1, n, stride=2), :]
        p0, p1 = pair(o0, o1)
        target_ref[pl.ds(2 * c, n, stride=side), :] = p0
        target_ref[pl.ds(2 * c + 1, n, stride=side), :] = p1

    low = first_half(side)

    def term_of(s, images):
        both = dot(l_ref[s], images)
        blurred = jnp.where(low, both[:side], both[side:]).astype(jnp.bfloat16)
        predicted = dot(blurred, q_ref[s])
        scale = jnp.where(
            low,
            weight_ref[0, 2 * s] * cover_ref[0, 2 * s].astype(jnp.float32),
            weight_ref[0, 2 * s + 1] * cover_ref[0, 2 * s + 1].astype(jnp.float32),
        )
        target = target_ref[pl.ds(pl.multiple_of(s * side, side), side), :]
        misfit = (scale * (predicted - target)).astype(jnp.bfloat16)
        both = dot(lt_ref[s], misfit)
        back = jnp.where(low, both[:side], both[side:]).astype(jnp.bfloat16)
        return dot_nt(back, q_ref[s]).astype(jnp.bfloat16)

    def answer(i):
        k = i + 1
        model_copy(k).wait_recv()
        term_out[k] = term_of(lax.rem(me - k + n, n), model_in[k])
        term_copy(k).start()

    each(n - 1, answer)
    term_in[me] = term_of(me, stage_ref[me * bands // n])

    def collect(i):
        k = i + 1
        source = lax.rem(me + k, n)
        pltpu.make_async_remote_copy(
            src_ref=term_out.at[k],
            dst_ref=term_in.at[source],
            send_sem=term_send.at[k],
            recv_sem=term_recv.at[source],
            device_id={"epoch": source},
            device_id_type=MESH,
        ).wait_recv()

    each(n - 1, collect)

    def factor(i):
        shared = jnp.full((side // 2, LANES), count_ref[0, i], jnp.int32)
        return step_size / shared.astype(jnp.float32)

    f0, f1 = factor(0), factor(1)
    for c in range(bands):
        total = jnp.zeros((side, LANES), jnp.float32)
        for e in range(n):
            if e * bands // n == c:
                total = total + term_in[e].astype(jnp.float32)
        wide_ref[c * side : (c + 1) * side, :] = total
        even = pl.ds(c * side, side // 2, stride=2)
        odd = pl.ds(c * side + 1, side // 2, stride=2)
        g0, g1 = pair(wide_ref[even, :], wide_ref[odd, :])
        out_ref[even, :] = models_ref[even, :] - f0 * g0
        out_ref[odd, :] = models_ref[odd, :] - f1 * g1

    def drain(i):
        model_copy(i + 1).wait_send()
        term_copy(i + 1).wait_send()

    each(n - 1, drain)


def on_device(
    models, observed, weights, coverage, offsets, counts, psf_y, resample_y, psf_x, resample_x
):
    n = lax.axis_size("epoch")
    _, per, bands, pixels = models.shape
    side = round(pixels**0.5)
    assert per * side == LANES and observed.shape[0] == 1 and observed.shape[1] == per * n
    vmem = pl.BlockSpec(memory_space=pltpu.VMEM)
    smem = pl.BlockSpec(memory_space=pltpu.SMEM)
    half = jnp.bfloat16
    chunks = pixels // LANES
    rows = models[0].reshape(per, bands, chunks, LANES).transpose(1, 2, 0, 3)
    updated = pl.pallas_call(
        functools.partial(kernel, n),
        out_shape=jax.ShapeDtypeStruct((bands * side, LANES), jnp.float32),
        in_specs=[vmem, vmem, smem, smem, smem, smem, vmem, vmem, vmem, vmem],
        out_specs=vmem,
        scratch_shapes=[
            pltpu.VMEM((bands * side, LANES), jnp.float32),
            pltpu.VMEM((bands, side, LANES), half),
            pltpu.VMEM((per * n * chunks, LANES), jnp.float32),
            pltpu.VMEM((n * side, LANES), jnp.float32),
            pltpu.VMEM((chunks, LANES), jnp.float32),
            pltpu.VMEM((side, side), jnp.float32),
            pltpu.VMEM((n, 2 * side, side), half),
            pltpu.VMEM((n, 2 * side, side), half),
            pltpu.VMEM((n, LANES, LANES), half),
            pltpu.VMEM((n, side, LANES), half),
            pltpu.VMEM((n, side, LANES), half),
            pltpu.VMEM((n, side, LANES), half),
            pltpu.SemaphoreType.DMA((n,)),
            pltpu.SemaphoreType.DMA((n,)),
            pltpu.SemaphoreType.DMA((n,)),
            pltpu.SemaphoreType.DMA((n,)),
        ],
        compiler_params=pltpu.CompilerParams(collective_id=0, has_side_effects=True),
    )(
        rows.reshape(bands * side, LANES),
        observed[0],
        weights,
        coverage,
        offsets[0].T,
        counts,
        psf_y,
        resample_y,
        psf_x,
        resample_x,
    )
    updated = updated.reshape(bands, chunks, per, LANES).transpose(2, 0, 1, 3)
    return updated.reshape(models.shape)


def solution(mesh):
    return jax.shard_map(
        on_device,
        mesh=mesh,
        in_specs=(
            P("blend", "epoch", None, None),
            P("epoch", "blend", None),
            P("epoch", "blend"),
            P("epoch", "blend"),
            P("epoch", "blend", None),
            P("blend", "epoch"),
            P("epoch", None),
            P("epoch", None),
            P("epoch", None),
            P("epoch", None),
        ),
        out_specs=P("blend", "epoch", None, None),
        check_vma=False,
    )
```

```python
import functools

import jax
import jax.numpy as jnp
from jax import lax
from jax.experimental import pallas as pl
from jax.experimental.pallas import tpu as pltpu
from jax.sharding import PartitionSpec as P

step_size = 0.5
LANES = 128
UNROLL = 8
MESH = pl.DeviceIdType.MESH


def dot(a, b):
    return jnp.dot(a, b, preferred_element_type=jnp.float32)


def dot_nt(a, b):
    return lax.dot_general(a, b, (((1,), (1,)), ((), ())), preferred_element_type=jnp.float32)


def each(count, body):
    if count <= UNROLL:
        for step in range(count):
            body(step)
    else:

        @pl.loop(0, count)
        def _(step):
            body(step)


def kernel(
    n,
    *refs,
):
    count = 10
    held = refs[count + 1 : 2 * count + 1]
    loads = [
        pltpu.make_async_copy(refs[i], held[i], refs[2 * count + 1].at[i]) for i in range(count)
    ]
    body(n, loads, *held, refs[count], *refs[2 * count + 2 :])


def body(
    n,
    loads,
    models_ref,
    obs_ref,
    weight_ref,
    cover_ref,
    off_ref,
    count_ref,
    psf_y_ref,
    res_y_ref,
    psf_x_ref,
    res_x_ref,
    out_ref,
    wide_ref,
    stage_ref,
    tmp_ref,
    target_ref,
    flat_ref,
    square_ref,
    l_ref,
    lt_ref,
    q_ref,
    model_in,
    term_out,
    term_in,
    model_send,
    model_recv,
    term_send,
    term_recv,
):
    bands, side = stage_ref.shape[0], stage_ref.shape[1]
    chunks = psf_y_ref.shape[1] // LANES
    me = lax.axis_index("epoch")

    barrier = pltpu.get_barrier_semaphore()

    def greet(k):
        pl.semaphore_signal(
            barrier, inc=1, device_id={"epoch": lax.rem(me + k + 1, n)}, device_id_type=MESH
        )

    each(n - 1, greet)
    for load in loads:
        load.start()

    def first_half(rows):
        return lax.broadcasted_iota(jnp.int32, (rows, LANES), 1) < side

    def pair(even, odd):
        low = first_half(even.shape[0])
        return (
            jnp.where(low, even, pltpu.roll(odd, side, 1)),
            jnp.where(low, pltpu.roll(even, side, 1), odd),
        )

    loads[0].wait()
    for c in range(bands):
        even = pl.ds(c * side, side // 2, stride=2)
        odd = pl.ds(c * side + 1, side // 2, stride=2)
        wide_ref[even, :], wide_ref[odd, :] = pair(models_ref[even, :], models_ref[odd, :])
        stage_ref[c] = wide_ref[c * side : (c + 1) * side, :].astype(jnp.bfloat16)

    pl.semaphore_wait(barrier, n - 1)

    def model_copy(k):
        dest = lax.rem(me + k, n)
        return pltpu.make_async_remote_copy(
            src_ref=stage_ref.at[dest * bands // n],
            dst_ref=model_in.at[k],
            send_sem=model_send.at[k],
            recv_sem=model_recv.at[k],
            device_id={"epoch": dest},
            device_id_type=MESH,
        )

    def term_copy(k):
        return pltpu.make_async_remote_copy(
            src_ref=term_out.at[k],
            dst_ref=term_in.at[me],
            send_sem=term_send.at[k],
            recv_sem=term_recv.at[me],
            device_id={"epoch": lax.rem(me - k + n, n)},
            device_id_type=MESH,
        )

    each(n - 1, lambda i: model_copy(n - 1 - i).start())

    for load in loads[1:]:
        load.wait()

    def square(ref):
        for c in range(chunks):
            flat_ref[c : c + 1, :] = ref[:, c * LANES : (c + 1) * LANES].astype(jnp.float32)
        square_ref[pl.ds(0, chunks, stride=2), :] = flat_ref[:, :side]
        square_ref[pl.ds(1, chunks, stride=2), :] = flat_ref[:, side:]
        return square_ref[...].astype(jnp.bfloat16)

    left = dot(square(psf_y_ref), square(res_y_ref)).astype(jnp.bfloat16)
    right = dot(square(psf_x_ref), square(res_x_ref)).astype(jnp.bfloat16)
    right_twice = jnp.concatenate([right, right], axis=0)
    row = lax.broadcasted_iota(jnp.int32, (2 * side, side), 0)
    col = lax.broadcasted_iota(jnp.int32, (2 * side, side), 1)
    turn = lax.rem(row - col + side, side)
    top = row < side
    diagonal = (lax.broadcasted_iota(jnp.int32, (LANES, LANES), 0) < side) == (
        lax.broadcasted_iota(jnp.int32, (LANES, LANES), 1) < side
    )

    def operators(s):
        def picks(axis):
            moved = jnp.where(top, off_ref[axis, 2 * s], off_ref[axis, 2 * s + 1])
            return jnp.where(turn == moved, 1.0, 0.0).astype(jnp.bfloat16)

        down, across = picks(0), picks(1)
        lt_ref[s] = dot_nt(down, left).astype(jnp.bfloat16)
        l_ref[s, :side] = dot_nt(left, down[:side]).astype(jnp.bfloat16)
        l_ref[s, side:] = dot_nt(left, down[side:]).astype(jnp.bfloat16)
        q_ref[s] = jnp.where(diagonal, dot_nt(across, right_twice), 0.0).astype(jnp.bfloat16)

    each(n, operators)

    for c in range(chunks):
        at = c * 2 * n
        tmp_ref[at : at + 2 * n, :] = obs_ref[:, c * LANES : (c + 1) * LANES].astype(jnp.float32)
        o0 = tmp_ref[pl.ds(at, n, stride=2), :]
        o1 = tmp_ref[pl.ds(at + 1, n, stride=2), :]
        p0, p1 = pair(o0, o1)
        target_ref[pl.ds(2 * c, n, stride=side), :] = p0
        target_ref[pl.ds(2 * c + 1, n, stride=side), :] = p1

    low = first_half(side)

    def term_of(s, images):
        both = dot(l_ref[s], images)
        blurred = jnp.where(low, both[:side], both[side:]).astype(jnp.bfloat16)
        predicted = dot(blurred, q_ref[s])
        scale = jnp.where(
            low,
            weight_ref[0, 2 * s] * cover_ref[0, 2 * s].astype(jnp.float32),
            weight_ref[0, 2 * s + 1] * cover_ref[0, 2 * s + 1].astype(jnp.float32),
        )
        target = target_ref[pl.ds(pl.multiple_of(s * side, side), side), :]
        misfit = (scale * (predicted - target)).astype(jnp.bfloat16)
        both = dot(lt_ref[s], misfit)
        back = jnp.where(low, both[:side], both[side:]).astype(jnp.bfloat16)
        return dot_nt(back, q_ref[s]).astype(jnp.bfloat16)

    def answer(i):
        k = i + 1
        model_copy(k).wait_recv()
        term_out[k] = term_of(lax.rem(me - k + n, n), model_in[k])
        term_copy(k).start()

    each(n - 1, answer)
    term_in[me] = term_of(me, stage_ref[me * bands // n])

    def collect(i):
        k = i + 1
        source = lax.rem(me + k, n)
        pltpu.make_async_remote_copy(
            src_ref=term_out.at[k],
            dst_ref=term_in.at[source],
            send_sem=term_send.at[k],
            recv_sem=term_recv.at[source],
            device_id={"epoch": source},
            device_id_type=MESH,
        ).wait_recv()

    each(n - 1, collect)

    def factor(i):
        shared = jnp.full((side // 2, LANES), count_ref[0, i], jnp.int32)
        return step_size / shared.astype(jnp.float32)

    f0, f1 = factor(0), factor(1)
    for c in range(bands):
        total = jnp.zeros((side, LANES), jnp.float32)
        for e in range(n):
            if e * bands // n == c:
                total = total + term_in[e].astype(jnp.float32)
        wide_ref[c * side : (c + 1) * side, :] = total
        even = pl.ds(c * side, side // 2, stride=2)
        odd = pl.ds(c * side + 1, side // 2, stride=2)
        g0, g1 = pair(wide_ref[even, :], wide_ref[odd, :])
        out_ref[even, :] = models_ref[even, :] - f0 * g0
        out_ref[odd, :] = models_ref[odd, :] - f1 * g1

    def drain(i):
        model_copy(i + 1).wait_send()
        term_copy(i + 1).wait_send()

    each(n - 1, drain)


def on_device(
    models, observed, weights, coverage, offsets, counts, psf_y, resample_y, psf_x, resample_x
):
    n = lax.axis_size("epoch")
    _, per, bands, pixels = models.shape
    side = round(pixels**0.5)
    assert per * side == LANES and observed.shape[0] == 1 and observed.shape[1] == per * n
    half = jnp.bfloat16
    chunks = pixels // LANES
    rows = models[0].reshape(per, bands, chunks, LANES).transpose(1, 2, 0, 3)
    operands = (
        rows.reshape(bands * side, LANES),
        observed[0],
        weights,
        coverage,
        offsets[0].T,
        counts,
        psf_y,
        resample_y,
        psf_x,
        resample_x,
    )
    scalars = range(2, 6)
    updated = pl.pallas_call(
        functools.partial(kernel, n),
        out_shape=pltpu.VMEM((bands * side, LANES), jnp.float32),
        in_specs=[pl.BlockSpec(memory_space=pltpu.HBM)] * len(operands),
        out_specs=pl.BlockSpec(memory_space=pltpu.VMEM),
        scratch_shapes=[
            (pltpu.SMEM if i in scalars else pltpu.VMEM)(x.shape, x.dtype)
            for i, x in enumerate(operands)
        ]
        + [
            pltpu.SemaphoreType.DMA((len(operands),)),
            pltpu.VMEM((bands * side, LANES), jnp.float32),
            pltpu.VMEM((bands, side, LANES), half),
            pltpu.VMEM((per * n * chunks, LANES), jnp.float32),
            pltpu.VMEM((n * side, LANES), jnp.float32),
            pltpu.VMEM((chunks, LANES), jnp.float32),
            pltpu.VMEM((side, side), jnp.float32),
            pltpu.VMEM((n, 2 * side, side), half),
            pltpu.VMEM((n, 2 * side, side), half),
            pltpu.VMEM((n, LANES, LANES), half),
            pltpu.VMEM((n, side, LANES), half),
            pltpu.VMEM((n, side, LANES), half),
            pltpu.VMEM((n, side, LANES), half),
            pltpu.SemaphoreType.DMA((n,)),
            pltpu.SemaphoreType.DMA((n,)),
            pltpu.SemaphoreType.DMA((n,)),
            pltpu.SemaphoreType.DMA((n,)),
        ],
        compiler_params=pltpu.CompilerParams(collective_id=0, vmem_limit_bytes=32 * 2**20, has_side_effects=True),
    )(*[pltpu.with_memory_space_constraint(x, pltpu.HBM) for x in operands])
    updated = updated.reshape(bands, chunks, per, LANES).transpose(2, 0, 1, 3)
    return updated.reshape(models.shape)


def solution(mesh):
    return jax.shard_map(
        on_device,
        mesh=mesh,
        in_specs=(
            P("blend", "epoch", None, None),
            P("epoch", "blend", None),
            P("epoch", "blend"),
            P("epoch", "blend"),
            P("epoch", "blend", None),
            P("blend", "epoch"),
            P("epoch", None),
            P("epoch", None),
            P("epoch", None),
            P("epoch", None),
        ),
        out_specs=P("blend", "epoch", None, None),
        check_vma=False,
    )
```

```python
import functools

import jax
import jax.numpy as jnp
from jax import lax
from jax.experimental import pallas as pl
from jax.experimental.pallas import tpu as pltpu
from jax.sharding import PartitionSpec as P

step_size = 0.5
LANES = 128
UNROLL = 8
GROUP = 7
MESH = pl.DeviceIdType.MESH


def dot(a, b):
    return jnp.dot(a, b, preferred_element_type=jnp.float32)


def dot_nt(a, b):
    return lax.dot_general(a, b, (((1,), (1,)), ((), ())), preferred_element_type=jnp.float32)


def each(count, body):
    if count <= UNROLL:
        for step in range(count):
            body(step)
    else:

        @pl.loop(0, count)
        def _(step):
            body(step)


def kernel(
    n,
    nb,
    *refs,
):
    count = 10
    held = refs[count + 1 : 2 * count + 1]
    loads = [
        pltpu.make_async_copy(refs[i], held[i], refs[2 * count + 1].at[i]) for i in range(count)
    ]
    body(n, nb, loads, *held, refs[count], *refs[2 * count + 2 :])


def body(
    n,
    nb,
    loads,
    models_ref,
    obs_ref,
    weight_ref,
    cover_ref,
    off_ref,
    count_ref,
    psf_y_ref,
    res_y_ref,
    psf_x_ref,
    res_x_ref,
    out_ref,
    wide_ref,
    stage_ref,
    tmp_ref,
    target_ref,
    flat_ref,
    square_ref,
    mats,
    seen_out,
    seen_in,
    term_ref,
    mats_send,
    mats_recv,
    seen_send,
    seen_recv,
    relay_send,
    relay_recv,
):
    bands, side = stage_ref.shape[0], mats.shape[1]
    chunks = psf_y_ref.shape[1] // LANES
    me, mine = lax.axis_index("epoch"), lax.axis_index("blend")
    part = pl.ds(pl.multiple_of(mine * (side // nb), side // nb), side // nb)

    barrier = pltpu.get_barrier_semaphore()

    def greet(k):
        pl.semaphore_signal(
            barrier, inc=1, device_id={"epoch": lax.rem(me + k + 1, n)}, device_id_type=MESH
        )

    def greet_twin(k):
        pl.semaphore_signal(
            barrier, inc=1, device_id={"blend": lax.rem(mine + k + 1, nb)}, device_id_type=MESH
        )

    each(n - 1, greet)
    each(nb - 1, greet_twin)
    for load in loads:
        load.start()

    def first_half(rows):
        return lax.broadcasted_iota(jnp.int32, (rows, LANES), 1) < side

    def pair(even, odd):
        low = first_half(even.shape[0])
        return (
            jnp.where(low, even, pltpu.roll(odd, side, 1)),
            jnp.where(low, pltpu.roll(even, side, 1), odd),
        )

    def square(ref):
        for c in range(chunks):
            flat_ref[c : c + 1, :] = ref[:, c * LANES : (c + 1) * LANES].astype(jnp.float32)
        square_ref[pl.ds(0, chunks, stride=2), :] = flat_ref[:, :side]
        square_ref[pl.ds(1, chunks, stride=2), :] = flat_ref[:, side:]
        return square_ref[...].astype(jnp.bfloat16)

    for load in loads[6:]:
        load.wait()
    left = dot(square(psf_y_ref), square(res_y_ref))
    right = dot(square(psf_x_ref), square(res_x_ref))
    mats[me] = jnp.concatenate([left, right], axis=1).astype(jnp.bfloat16)

    for load in loads[1:6]:
        load.wait()
    for c in range(chunks):
        at = c * 2 * n
        tmp_ref[at : at + 2 * n, :] = obs_ref[:, c * LANES : (c + 1) * LANES].astype(jnp.float32)
        o0 = tmp_ref[pl.ds(at, n, stride=2), :]
        o1 = tmp_ref[pl.ds(at + 1, n, stride=2), :]
        p0, p1 = pair(o0, o1)
        target_ref[pl.ds(2 * c, n, stride=side), :] = p0
        target_ref[pl.ds(2 * c + 1, n, stride=side), :] = p1

    notes = seen_out.shape[1] - side
    line = lax.broadcasted_iota(jnp.int32, (notes, LANES), 0)
    low = first_half(notes)

    def pack(d):
        rows = pl.ds(pl.multiple_of(d * side, side), side)
        seen_out[d, :side] = target_ref[rows, :].astype(jnp.bfloat16)
        scale = jnp.where(
            low,
            weight_ref[0, 2 * d] * cover_ref[0, 2 * d].astype(jnp.float32),
            weight_ref[0, 2 * d + 1] * cover_ref[0, 2 * d + 1].astype(jnp.float32),
        )
        high = scale.astype(jnp.bfloat16).astype(jnp.float32)
        mid = (scale - high).astype(jnp.bfloat16).astype(jnp.float32)
        values = [off_ref[axis, 2 * d + i].astype(jnp.float32) for axis in (0, 1) for i in (0, 1)]
        note = jnp.zeros((notes, LANES), jnp.float32)
        for i, value in enumerate(values + [high, mid, scale - high - mid]):
            note = jnp.where(line == i, value, note)
        seen_out[d, side:] = note.astype(jnp.bfloat16)

    each(n, pack)

    pl.semaphore_wait(barrier, n + nb - 2)

    upper = me < n // 2
    longer = jnp.where(upper, n - 1 - me, me)

    def peer(j):
        first = jnp.where(upper, n - 1 - j, j)
        second = jnp.where(upper, j - longer, n - 1 - (j - longer))
        return jnp.where(j < longer, first, second)

    def mats_copy(dest):
        return pltpu.make_async_remote_copy(
            src_ref=mats.at[me, part],
            dst_ref=mats.at[me, part],
            send_sem=mats_send.at[dest],
            recv_sem=mats_recv.at[me],
            device_id={"epoch": dest},
            device_id_type=MESH,
        )

    def mats_arrival(source):
        return pltpu.make_async_remote_copy(
            src_ref=mats.at[source, part],
            dst_ref=mats.at[source, part],
            send_sem=mats_send.at[source],
            recv_sem=mats_recv.at[source],
            device_id={"epoch": source},
            device_id_type=MESH,
        )

    def seen_copy(dest):
        return pltpu.make_async_remote_copy(
            src_ref=seen_out.at[dest],
            dst_ref=seen_in.at[me],
            send_sem=seen_send.at[dest],
            recv_sem=seen_recv.at[me],
            device_id={"epoch": dest},
            device_id_type=MESH,
        )

    def seen_arrival(source):
        return pltpu.make_async_remote_copy(
            src_ref=seen_out.at[source],
            dst_ref=seen_in.at[source],
            send_sem=seen_send.at[source],
            recv_sem=seen_recv.at[source],
            device_id={"epoch": source},
            device_id_type=MESH,
        )

    def relay_copy(source, k):
        return pltpu.make_async_remote_copy(
            src_ref=mats.at[source, part],
            dst_ref=mats.at[source, part],
            send_sem=relay_send.at[k * n + source],
            recv_sem=relay_recv.at[k * n + source],
            device_id={"blend": lax.rem(mine + k, nb)},
            device_id_type=MESH,
        )

    def relay_arrival(source, k):
        twin = lax.rem(mine - k + nb, nb)
        piece = pl.ds(pl.multiple_of(twin * (side // nb), side // nb), side // nb)
        return pltpu.make_async_remote_copy(
            src_ref=mats.at[source, piece],
            dst_ref=mats.at[source, piece],
            send_sem=relay_send.at[k * n + source],
            recv_sem=relay_recv.at[k * n + source],
            device_id={"blend": twin},
            device_id_type=MESH,
        )

    each(n - 1, lambda j: mats_copy(peer(j)).start())
    each(n - 1, lambda j: seen_copy(peer(j)).start())

    low = first_half(side)
    loads[0].wait()
    for c in range(bands):
        even = pl.ds(c * side, side // 2, stride=2)
        odd = pl.ds(c * side + 1, side // 2, stride=2)
        wide_ref[even, :], wide_ref[odd, :] = pair(models_ref[even, :], models_ref[odd, :])
        both = wide_ref[c * side : (c + 1) * side, :]
        stage_ref[c, :side] = jnp.where(low, both, 0.0).astype(jnp.bfloat16)
        stage_ref[c, side:] = jnp.where(low, 0.0, both).astype(jnp.bfloat16)

    row = lax.broadcasted_iota(jnp.int32, (LANES, LANES), 0)
    col = lax.broadcasted_iota(jnp.int32, (LANES, LANES), 1)
    turn = lax.rem(row - col + LANES, side).astype(jnp.float32)
    top, front = row < side, col < side
    diagonal = top == front

    def terms_of(pairs):
        epochs = [e for e, _ in pairs]
        seen = [ref[at] for _, (ref, at) in pairs]
        notes_of = [x[side:].astype(jnp.float32) for x in seen]
        both = [mats[e] for e in epochs]

        def picks(note, first, lanes):
            moved = jnp.where(top, note[first : first + 1], note[first + 1 : first + 2])
            hit = jnp.logical_and(turn == moved, lanes)
            return jnp.where(hit, 1.0, 0.0).astype(jnp.bfloat16)

        down = [picks(x, 0, front) for x in notes_of]
        left = [dot_nt(m, d).astype(jnp.bfloat16) for m, d in zip(both, down)]
        blurred = [
            dot(x, stage_ref[e * bands // n]).astype(jnp.bfloat16) for x, e in zip(left, epochs)
        ]
        across = [picks(x, 2, jnp.logical_not(front)) for x in notes_of]
        right = [
            jnp.where(diagonal, dot_nt(a, jnp.concatenate([m, m], axis=0)), 0.0).astype(
                jnp.bfloat16
            )
            for a, m in zip(across, both)
        ]
        predicted = [dot(x, r) for x, r in zip(blurred, right)]
        left_t = [dot_nt(d, m).astype(jnp.bfloat16) for m, d in zip(both, down)]
        misfit = [
            ((x[4:5] + x[5:6] + x[6:7]) * (p - o[:side].astype(jnp.float32))).astype(jnp.bfloat16)
            for x, p, o in zip(notes_of, predicted, seen)
        ]
        back = [dot(t, x) for t, x in zip(left_t, misfit)]
        back = [jnp.where(low, x[:side], x[side:]).astype(jnp.bfloat16) for x in back]
        terms = [dot_nt(x, r) for x, r in zip(back, right)]
        for e, term in zip(epochs, terms):
            term_ref[e] = term

    terms_of([(me, (seen_out, me))])

    def relay(j):
        source = peer(n - 2 - j)
        mats_arrival(source).wait_recv()
        for k in range(1, nb):
            relay_copy(source, k).start()

    def absorb(js):
        sources = [peer(n - 2 - j) for j in js]
        for source in sources:
            for k in range(1, nb):
                relay_arrival(source, k).wait_recv()
            seen_arrival(source).wait_recv()
        terms_of([(source, (seen_in, source)) for source in sources])

    each(n - 1, relay)
    if n <= UNROLL:
        for first in range(0, n - 1, GROUP):
            absorb(range(first, min(first + GROUP, n - 1)))
    else:
        each(n - 1, lambda j: absorb([j]))

    def factor(i):
        shared = jnp.full((side // 2, LANES), count_ref[0, i], jnp.int32)
        return step_size / shared.astype(jnp.float32)

    f0, f1 = factor(0), factor(1)
    for c in range(bands):
        total = jnp.zeros((side, LANES), jnp.float32)
        for e in range(n):
            if e * bands // n == c:
                total = total + term_ref[e]
        wide_ref[c * side : (c + 1) * side, :] = total
        even = pl.ds(c * side, side // 2, stride=2)
        odd = pl.ds(c * side + 1, side // 2, stride=2)
        g0, g1 = pair(wide_ref[even, :], wide_ref[odd, :])
        out_ref[even, :] = models_ref[even, :] - f0 * g0
        out_ref[odd, :] = models_ref[odd, :] - f1 * g1

    def drain(j):
        mats_copy(peer(j)).wait_send()
        seen_copy(peer(j)).wait_send()
        for k in range(1, nb):
            relay_copy(peer(j), k).wait_send()

    each(n - 1, drain)


def on_device(
    models, observed, weights, coverage, offsets, counts, psf_y, resample_y, psf_x, resample_x
):
    n, nb = lax.axis_size("epoch"), lax.axis_size("blend")
    _, per, bands, pixels = models.shape
    side = round(pixels**0.5)
    assert per * side == LANES and observed.shape[0] == 1 and observed.shape[1] == per * n
    half = jnp.bfloat16
    chunks = pixels // LANES
    rows = models[0].reshape(per, bands, chunks, LANES).transpose(1, 2, 0, 3)
    operands = (
        rows.reshape(bands * side, LANES),
        observed[0],
        weights,
        coverage,
        offsets[0].T,
        counts,
        psf_y,
        resample_y,
        psf_x,
        resample_x,
    )
    scalars = range(2, 6)
    updated = pl.pallas_call(
        functools.partial(kernel, n, nb),
        out_shape=pltpu.VMEM((bands * side, LANES), jnp.float32),
        in_specs=[pl.BlockSpec(memory_space=pltpu.HBM)] * len(operands),
        out_specs=pl.BlockSpec(memory_space=pltpu.VMEM),
        scratch_shapes=[
            (pltpu.SMEM if i in scalars else pltpu.VMEM)(x.shape, x.dtype)
            for i, x in enumerate(operands)
        ]
        + [
            pltpu.SemaphoreType.DMA((len(operands),)),
            pltpu.VMEM((bands * side, LANES), jnp.float32),
            pltpu.VMEM((bands, LANES, LANES), half),
            pltpu.VMEM((per * n * chunks, LANES), jnp.float32),
            pltpu.VMEM((n * side, LANES), jnp.float32),
            pltpu.VMEM((chunks, LANES), jnp.float32),
            pltpu.VMEM((side, side), jnp.float32),
            pltpu.VMEM((n, side, LANES), half),
            pltpu.VMEM((n, side + 16, LANES), half),
            pltpu.VMEM((n, side + 16, LANES), half),
            pltpu.VMEM((n, side, LANES), jnp.float32),
            pltpu.SemaphoreType.DMA((n,)),
            pltpu.SemaphoreType.DMA((n,)),
            pltpu.SemaphoreType.DMA((n,)),
            pltpu.SemaphoreType.DMA((n,)),
            pltpu.SemaphoreType.DMA((nb * n,)),
            pltpu.SemaphoreType.DMA((nb * n,)),
        ],
        compiler_params=pltpu.CompilerParams(collective_id=0, vmem_limit_bytes=32 * 2**20, has_side_effects=True),
    )(*[pltpu.with_memory_space_constraint(x, pltpu.HBM) for x in operands])
    updated = updated.reshape(bands, chunks, per, LANES).transpose(2, 0, 1, 3)
    return updated.reshape(models.shape)


def solution(mesh):
    return jax.shard_map(
        on_device,
        mesh=mesh,
        in_specs=(
            P("blend", "epoch", None, None),
            P("epoch", "blend", None),
            P("epoch", "blend"),
            P("epoch", "blend"),
            P("epoch", "blend", None),
            P("blend", "epoch"),
            P("epoch", None),
            P("epoch", None),
            P("epoch", None),
            P("epoch", None),
        ),
        out_specs=P("blend", "epoch", None, None),
        check_vma=False,
    )
```
